32 devices in a mesh: row: 4 (over y, core), col: 8 (over z, x).
Axes of the slice: x: 2, y: 2, z: 4, core: 2. Of those that a mesh axis runs over, the one named last changes fastest.
Arguments:
- matrix: float32 [16384, 16384], P('row', 'col'), as said below
Outputs:
- hess_panel: float32 [16384, 8], P('row')
- reflectors: float32 [16384, 8], P('row')
- wy_products: float32 [16384, 8], P('row')
- wy_factor: float32 [8, 8], replicated
Inputs may be any that keep to these rules, and one draw needn't show every extreme that they name: Entries matrix[i+1, i] lie within 2.5 +- 6 / sqrt(16384); every other entry within +- 6 / sqrt(16384).
All inputs are finite; a program needn't handle non-finite values.
Results may differ from the reference program's by a relative error of at most 0.0003.
Values sent between devices are 32-bit elements; how exact they have to be, the bound alone decides.
A program may use at most 128 MiB of HBM per device.

```python
import math
import jax
import jax.numpy as jnp
from jax import lax

N = 16384
NB = 8


def draw_matrix(key, part):
    first = jax.random.fold_in(key, 11)
    base = jax.random.truncated_normal(first, -6.0, 6.0, (N, N), jnp.float32)
    return base / math.sqrt(N) + 2.5 * jnp.eye(N, k=-1, dtype=jnp.float32)


def setup_inputs(seed: int = 0) -> dict:
    key_of = jax.random.split(jax.random.key(seed), 2)
    matrix = draw_matrix(jax.random.fold_in(key_of[1], 71), 0)
    return {"matrix": matrix}


def reference(matrix):
    exact = lax.Precision.HIGHEST
    order = matrix.shape[0]
    row_ids = jnp.arange(order, dtype=jnp.int32)
    refl = jnp.zeros((order, NB), jnp.float32)
    wy_prod = jnp.zeros((order, NB), jnp.float32)
    factor = jnp.zeros((NB, NB), jnp.float32)
    columns = []
    for column in range(NB):
        current = matrix[:, column] - jnp.dot(wy_prod, refl[column], precision=exact)
        inner = jnp.dot(current, refl, precision=exact)
        current = current - jnp.dot(refl, jnp.dot(inner, factor, precision=exact), precision=exact)
        masked = jnp.where(row_ids > column, current, jnp.float32(0.0))
        leading = current[column + 1]
        length = jnp.sqrt(jnp.sum(masked * masked))
        orient = jnp.where(leading >= 0, jnp.float32(1.0), jnp.float32(-1.0))
        pivot_value = -orient * length
        vector = masked + jnp.where(row_ids == column + 1, orient * length, jnp.float32(0.0))
        vector = vector / jnp.sqrt(length * (length + jnp.abs(leading)))
        coupling = jnp.dot(vector, refl, precision=exact)
        image = jnp.dot(matrix, vector, precision=exact)
        new_y = image - jnp.dot(wy_prod, coupling, precision=exact)
        new_t = -jnp.dot(factor, coupling, precision=exact)
        factor = factor.at[:, column].set(new_t).at[column, column].set(jnp.float32(1.0))
        wy_prod = wy_prod.at[:, column].set(new_y)
        refl = refl.at[:, column].set(vector)
        columns.append(jnp.where(row_ids <= column, current, jnp.where(row_ids == column + 1, pivot_value, jnp.float32(0.0))))
    return (jnp.stack(columns, axis=1), refl, wy_prod, factor)
```

```python
import functools

import jax
import jax.numpy as jnp
from jax import lax
from jax.experimental import pallas as pl
from jax.experimental.pallas import tpu as pltpu
from jax.sharding import PartitionSpec as P

NB = 8
LANES = 128
SUB = 8
CHUNK = LANES * SUB
BLOCK = 256
F32 = jnp.float32
BF16 = jnp.bfloat16


def kernel(
    nrow, ncol, a_hbm, hess_ref, refl_ref, wy_ref, fac_ref,
    a_ref, first_ref, pan_ref, mypan_ref, full_ref, vec_ref, part_ref, got_ref,
    out_ref, ymine_ref, dummy_ref,
    load_sem, first_sem, pan_send, pan_sem, rs_send, rs_sem, ag_send, ag_sem,
    y_send, y_sem,
):
    rows_local, cols_local = a_hbm.shape
    order = rows_local * nrow
    tiles = cols_local // LANES
    lines = rows_local // LANES
    owners = rows_local // CHUNK
    stride = ncol // owners
    row, col = lax.axis_index("row"), lax.axis_index("col")
    mine = col // stride
    is_owner = col - mine * stride == 0
    blocks = rows_local // BLOCK

    def wrap(value, bound):
        return jnp.where(value >= bound, value - bound, value)

    def peers_of_row(dr, act, skip):
        to_row = wrap(row + dr, nrow)
        for dc in range(1 if skip else 0, ncol):
            act(to_row, wrap(col + dc, ncol))

    def all_peers(act):
        def step(dr, carry):
            peers_of_row(dr, act, False)
            return carry

        lax.fori_loop(1, nrow, step, 0)
        peers_of_row(0, act, True)

    def block_load(i):
        span = pl.ds(i * BLOCK, BLOCK)
        return pltpu.make_async_copy(a_hbm.at[span], a_ref.at[span], load_sem.at[i])

    head = pltpu.make_async_copy(a_hbm.at[:, pl.ds(0, LANES)], first_ref, first_sem)

    @pl.when(col == 0)
    def _():
        head.start()

    for i in range(blocks):
        block_load(i).start()

    barrier = pltpu.get_barrier_semaphore()

    def greet(to_row, to_col):
        pl.semaphore_signal(
            barrier, inc=1, device_id=(to_row, to_col),
            device_id_type=pl.DeviceIdType.MESH,
        )

    all_peers(greet)
    pl.semaphore_wait(barrier, nrow * ncol - 1)

    def send(src, dst, send_sem, recv_sem, to_row, to_col):
        pltpu.make_async_remote_copy(
            src_ref=src, dst_ref=dst, send_sem=send_sem, recv_sem=recv_sem,
            device_id=(to_row, to_col), device_id_type=pl.DeviceIdType.MESH,
        ).start()

    def expect(ref, sem):
        pltpu.make_async_copy(ref, ref, sem).wait()

    @pl.when(col == 0)
    def _():
        head.wait()

        def turn(t, carry):
            block = first_ref[pl.ds(pl.multiple_of(t * LANES, LANES), LANES), :].T
            for k in range(NB):
                pan_ref[k, pl.ds(t, 1), :] = block[k : k + 1, :]
            return carry

        lax.fori_loop(0, lines, turn, 0)
        for q in range(1, owners):
            send(
                pan_ref.at[:, pl.ds(q * SUB, SUB)], mypan_ref, pan_send, pan_sem,
                row, jnp.int32(q * stride),
            )
        pltpu.make_async_copy(pan_ref.at[:, pl.ds(0, SUB)], mypan_ref, pan_sem).start()

    span = pl.ds(pl.multiple_of((row * owners + mine) * SUB, SUB), SUB)

    def gather(j):
        dst = full_ref.at[j, span]
        all_peers(
            lambda to_row, to_col: send(
                out_ref.at[j], dst, ag_send.at[j], ag_sem.at[j], to_row, to_col
            )
        )
        pltpu.make_async_copy(out_ref.at[j], dst, ag_sem.at[j]).start()

    @pl.when(is_owner)
    def _():
        expect(mypan_ref, pan_sem)
        out_ref[0] = mypan_ref[0]
        gather(0)

    ids = lax.broadcasted_iota(jnp.int32, (order // LANES, LANES), 0) * LANES
    ids = ids + lax.broadcasted_iota(jnp.int32, (order // LANES, LANES), 1)
    ones = jnp.ones((SUB, 2 * LANES), BF16)

    def total(value):
        return jnp.sum(jnp.sum(value, axis=0, keepdims=True), axis=1, keepdims=True)

    def fold(acc, t, j):
        high = acc.astype(BF16)
        low = (acc - high.astype(F32)).astype(BF16)
        both = jnp.concatenate([high, low], axis=1)
        res = lax.dot_general(
            ones, both, (((1,), (1,)), ((), ())), preferred_element_type=F32
        )
        part_ref[j, pl.ds(t, 1), :] = res[0:1, :]

    def matvec(j):
        base = col * tiles
        pieces = [
            jnp.broadcast_to(vec_ref[j, pl.ds(base + t, 1), :], (SUB, LANES))
            for t in range(tiles)
        ]

        def product(t):
            accs = []
            for s in range(LANES // SUB):
                at = pl.ds(pl.multiple_of(t * LANES + s * SUB, SUB), SUB)
                acc = a_ref[at, pl.ds(0, LANES)] * pieces[0]
                for p in range(1, tiles):
                    acc = acc + a_ref[at, pl.ds(p * LANES, LANES)] * pieces[p]
                accs.append(acc)
            return jnp.concatenate(accs, axis=0)

        per = BLOCK // LANES
        if j == 0:
            def loaded(i, carry):
                block_load(i).wait()
                for k in range(per):
                    fold(product(i * per + k), i * per + k, j)
                return carry

            lax.fori_loop(0, blocks, loaded, 0)
        else:
            def step(t, acc):
                fold(acc, t - 1, j)
                return product(t)

            fold(lax.fori_loop(1, lines, step, product(0)), lines - 1, j)

    factor = [[None] * NB for _ in range(NB)]
    local = pl.ds(pl.multiple_of(row * lines, SUB), lines)
    for j in range(NB):
        expect(full_ref.at[j], ag_sem.at[j])
        b = full_ref[j]
        if j > 0:
            inner = [total(vec_ref[k] * b) for k in range(j)]
            for m in range(j):
                weight = factor[0][m] * inner[0]
                for k in range(1, m + 1):
                    weight = weight + factor[k][m] * inner[k]
                b = b - vec_ref[m] * weight
        x = jnp.where(ids > j, b, F32(0.0))
        alpha = b[0:1, j + 1 : j + 2]
        norm = jnp.sqrt(total(x * x))
        signed = jnp.where(alpha >= 0, norm, -norm)
        u = x + jnp.where(ids == j + 1, signed, F32(0.0))
        u = u / jnp.sqrt(norm * (norm + jnp.abs(alpha)))
        vec_ref[j] = u
        matvec(j)
        for q in range(owners):
            @pl.when(jnp.logical_or(mine != q, jnp.logical_not(is_owner)))
            def _(q=q):
                send(
                    part_ref.at[j, pl.ds(q * SUB, SUB)], got_ref.at[j, col],
                    rs_send, rs_sem.at[j], row, jnp.int32(q * stride),
                )
        out_ref_h = jnp.where(ids <= j, b, jnp.where(ids == j + 1, -signed, F32(0.0)))
        full_ref[j] = out_ref_h
        hess_ref[j] = full_ref[j, local, :]
        refl_ref[j] = vec_ref[j, local, :]
        couple = [total(vec_ref[k] * u) for k in range(j)]
        for k in range(j):
            value = factor[k][k] * couple[k]
            for m in range(k + 1, j):
                value = value + factor[k][m] * couple[m]
            factor[k][j] = -value
        factor[j][j] = jnp.ones((1, 1), F32)
        if j + 1 < NB:
            edge = [vec_ref[k, 0:1, j + 1 : j + 2] for k in range(j + 1)]

        @pl.when(is_owner)
        def _():
            got_ref[j, pl.ds(col, 1)] = part_ref[
                j, pl.ds(pl.multiple_of(mine * SUB, SUB), SUB), :
            ][None]
            if j + 1 < NB:
                rest = mypan_ref[j + 1]
                for k in range(j):
                    rest = rest - ymine_ref[k] * edge[k]
            drop = jnp.zeros((SUB, LANES), F32)
            for k in range(j):
                drop = drop + ymine_ref[k] * couple[k]
            expect(got_ref.at[j, pl.ds(0, ncol - 1)], rs_sem.at[j])
            image = got_ref[j, 0]
            for i in range(1, ncol):
                image = image + got_ref[j, i]
            new_y = image - drop
            if j + 1 < NB:
                out_ref[j + 1] = rest - new_y * edge[j]
                gather(j + 1)
            ymine_ref[j] = new_y
            ydst = wy_ref.at[j, pl.ds(pl.multiple_of(mine * SUB, SUB), SUB)]
            peers_of_row(
                0,
                lambda to_row, to_col: send(
                    ymine_ref.at[j], ydst, y_send, y_sem, to_row, to_col
                ),
                True,
            )
            pltpu.make_async_copy(ymine_ref.at[j], ydst, y_sem).start()

    at_row = lax.broadcasted_iota(jnp.int32, (NB, NB), 0)
    at_col = lax.broadcasted_iota(jnp.int32, (NB, NB), 1)
    fac = jnp.zeros((NB, NB), F32)
    for k in range(NB):
        for m in range(k, NB):
            here = jnp.logical_and(at_row == k, at_col == m)
            fac = jnp.where(here, jnp.broadcast_to(factor[k][m], (NB, NB)), fac)
    fac_ref[...] = fac

    expect(wy_ref, y_sem)

    @pl.when(jnp.logical_not(is_owner))
    def _():
        expect(part_ref, rs_send)

    @pl.when(is_owner)
    def _():
        if owners > 1:
            expect(part_ref.at[:, pl.ds(0, (owners - 1) * SUB)], rs_send)
        for j in range(NB):
            expect(dummy_ref.at[pl.ds(0, (nrow * ncol - 1) * SUB)], ag_send.at[j])
        expect(dummy_ref.at[pl.ds(0, (ncol - 1) * SUB * NB)], y_send)

    if owners > 1:
        @pl.when(col == 0)
        def _():
            expect(pan_ref.at[:, pl.ds(0, (owners - 1) * SUB)], pan_send)


def shards(nrow, ncol, matrix):
    rows_local, cols_local = matrix.shape
    order = rows_local * nrow
    lines = rows_local // LANES
    tall = order // LANES
    blocks = rows_local // BLOCK
    panel = jax.ShapeDtypeStruct((NB, lines, LANES), F32)
    vmem = pl.BlockSpec(memory_space=pltpu.VMEM)
    dma = pltpu.SemaphoreType.DMA
    hess, refl, wy, fac = pl.pallas_call(
        functools.partial(kernel, nrow, ncol),
        out_shape=(panel, panel, panel, jax.ShapeDtypeStruct((NB, NB), F32)),
        in_specs=[pl.BlockSpec(memory_space=pl.ANY)],
        out_specs=(vmem, vmem, vmem, vmem),
        scratch_shapes=[
            pltpu.VMEM((rows_local, cols_local), F32),
            pltpu.VMEM((rows_local, LANES), F32),
            pltpu.VMEM((NB, lines, LANES), F32),
            pltpu.VMEM((NB, SUB, LANES), F32),
            pltpu.VMEM((NB, tall, LANES), F32),
            pltpu.VMEM((NB, tall, LANES), F32),
            pltpu.VMEM((NB, lines, LANES), F32),
            pltpu.VMEM((NB, ncol, SUB, LANES), F32),
            pltpu.VMEM((NB, SUB, LANES), F32),
            pltpu.VMEM((NB, SUB, LANES), F32),
            pltpu.VMEM((max(nrow * ncol - 1, (ncol - 1) * NB) * SUB, LANES), F32),
            dma((blocks,)),
            dma(()),
            dma(()),
            dma(()),
            dma(()),
            dma((NB,)),
            dma((NB,)),
            dma((NB,)),
            dma(()),
            dma(()),
        ],
        compiler_params=pltpu.CompilerParams(
            collective_id=0, has_side_effects=True, vmem_limit_bytes=56 * 2**20
        ),
    )(matrix)

    def lay(x):
        return x.reshape(NB, rows_local).T

    return lay(hess), lay(refl), lay(wy), fac


def solution(mesh):
    nrow, ncol = mesh.shape["row"], mesh.shape["col"]
    return jax.shard_map(
        functools.partial(shards, nrow, ncol),
        mesh=mesh,
        in_specs=(P("row", "col"),),
        out_specs=(P("row", None), P("row", None), P("row", None), P()),
        check_vma=False,
    )
```

```python
import functools

import jax
import jax.numpy as jnp
from jax import lax
from jax.experimental import pallas as pl
from jax.experimental.pallas import tpu as pltpu
from jax.sharding import PartitionSpec as P

NB = 8
LANES = 128
SUB = 8
STATS = 16
BLOCK = 256
F32 = jnp.float32
BF16 = jnp.bfloat16


def kernel(
    nrow, ncol, a_hbm, hess_ref, refl_ref, wy_ref, fac_ref,
    a_ref, first_ref, pan_ref, mypan_ref, part_ref, got_ref, stat_ref, stats_ref,
    vec_ref, yvec_ref,
    load_sem, first_sem, pan0_send, pan0_sem, pan_send, pan_sem, stat_send, stat_sem,
    part_send, part_sem, v_send, v_sem, y_send, y_sem,
):
    rows_local, cols_local = a_hbm.shape
    tiles = cols_local // LANES
    lines = rows_local // LANES
    split = rows_local // cols_local
    row, col = lax.axis_index("row"), lax.axis_index("col")
    blocks = rows_local // BLOCK

    def wrap(value, bound):
        return jnp.where(value >= bound, value - bound, value)

    def peers_of_row(dr, act, skip):
        to_row = wrap(row + dr, nrow)
        for dc in range(1 if skip else 0, ncol):
            act(to_row, wrap(col + dc, ncol))

    def block_load(i):
        span = pl.ds(i * BLOCK, BLOCK)
        return pltpu.make_async_copy(a_hbm.at[span], a_ref.at[span], load_sem.at[i])

    head = pltpu.make_async_copy(a_hbm.at[:, pl.ds(0, LANES)], first_ref, first_sem)

    @pl.when(col == 0)
    def _():
        head.start()

    for i in range(blocks):
        block_load(i).start()

    barrier = pltpu.get_barrier_semaphore()

    def greet(to_row, to_col):
        pl.semaphore_signal(
            barrier, inc=1, device_id=(to_row, to_col),
            device_id_type=pl.DeviceIdType.MESH,
        )

    def greet_row(dr, carry):
        peers_of_row(dr, greet, False)
        return carry

    lax.fori_loop(1, nrow, greet_row, 0)
    peers_of_row(0, greet, True)

    def send(src, dst, send_sem, recv_sem, to_row, to_col):
        pltpu.make_async_remote_copy(
            src_ref=src, dst_ref=dst, send_sem=send_sem, recv_sem=recv_sem,
            device_id=(to_row, to_col), device_id_type=pl.DeviceIdType.MESH,
        ).start()

    def place(src, dst, send_sem, recv_sem, to_row, to_col, here):
        @pl.when(here)
        def _():
            pltpu.make_async_copy(src, dst, recv_sem).start()

        @pl.when(jnp.logical_not(here))
        def _():
            send(src, dst, send_sem, recv_sem, to_row, to_col)

    def expect(ref, sem):
        pltpu.make_async_copy(ref, ref, sem).wait()

    def settle(ref, sem, here):
        count = ref.shape[1]

        @pl.when(jnp.logical_not(here))
        def _():
            expect(ref, sem)

        if count > 1:
            @pl.when(here)
            def _():
                expect(ref.at[:, pl.ds(0, count - 1)], sem)

    def spread(piece_of, dst, send_sem, recv_sem):
        for h in range(split):
            to_col = row * split + h
            for dr in range(nrow - 1, 0, -1):
                send(piece_of(h), dst, send_sem, recv_sem, wrap(row + dr, nrow), to_col)
            place(piece_of(h), dst, send_sem, recv_sem, row, to_col, to_col == col)

    @pl.when(col == 0)
    def _():
        head.wait()
        for h in range(split):
            def turn(t, carry):
                at = pl.multiple_of(h * cols_local + t * LANES, LANES)
                block = first_ref[pl.ds(at, LANES), :].T
                for k in range(NB + 1):
                    pan_ref[k, h, pl.ds(t, 1), :] = block[k : k + 1, :]
                return carry

            lax.fori_loop(0, tiles, turn, 0)

    pl.semaphore_wait(barrier, nrow * ncol - 1)

    @pl.when(col == 0)
    def _():
        spread(
            lambda h: pan_ref.at[pl.ds(0, 1), h], mypan_ref.at[pl.ds(0, 1)],
            pan0_send, pan0_sem,
        )
        spread(
            lambda h: pan_ref.at[pl.ds(1, NB), h], mypan_ref.at[pl.ds(1, NB)],
            pan_send, pan_sem,
        )

    ones = jnp.ones((SUB, 2 * LANES), BF16)

    def fold(acc, t, j):
        high = acc.astype(BF16)
        low = (acc - high.astype(F32)).astype(BF16)
        both = jnp.concatenate([high, low], axis=1)
        res = lax.dot_general(
            ones, both, (((1,), (1,)), ((), ())), preferred_element_type=F32
        )
        h = t // tiles
        part_ref[j, h, pl.ds(t - h * tiles, 1), :] = res[0:1, :]

    def matvec(j, vector):
        pieces = [
            jnp.broadcast_to(vector[t : t + 1, :], (SUB, LANES)) for t in range(tiles)
        ]

        def product(t):
            accs = []
            for s in range(LANES // SUB):
                at = pl.ds(pl.multiple_of(t * LANES + s * SUB, SUB), SUB)
                acc = a_ref[at, pl.ds(0, LANES)] * pieces[0]
                for p in range(1, tiles):
                    acc = acc + a_ref[at, pl.ds(p * LANES, LANES)] * pieces[p]
                accs.append(acc)
            return jnp.concatenate(accs, axis=0)

        per = BLOCK // LANES
        if j == 0:
            def loaded(i, carry):
                block_load(i).wait()
                for k in range(per):
                    fold(product(i * per + k), i * per + k, j)
                return carry

            lax.fori_loop(0, blocks, loaded, 0)
        else:
            def step(t, acc):
                fold(acc, t - 1, j)
                return product(t)

            fold(lax.fori_loop(1, lines, step, product(0)), lines - 1, j)

    owner = col // split
    slot = col - owner * split
    home = jnp.logical_and(owner == row, lax.rem(col, nrow) == row)

    def publish(src, ref, j, send_sem, recv_sem):
        for i in range(split):
            to_col = row + nrow * i
            here = jnp.logical_and(owner == row, to_col == col)
            place(src, ref.at[j, slot], send_sem, recv_sem, owner, to_col, here)

    lane = lax.broadcasted_iota(jnp.int32, (1, LANES), 1)
    line_ids = lax.broadcasted_iota(jnp.int32, (tiles, LANES), 0) * LANES
    ids = line_ids + lax.broadcasted_iota(jnp.int32, (tiles, LANES), 1)
    ids = ids + col * cols_local
    hess_ref[...] = jnp.zeros_like(hess_ref)

    factor = [[None] * NB for _ in range(NB)]
    gram = [[None] * NB for _ in range(NB)]
    tops = []
    images = []
    expect(mypan_ref.at[pl.ds(0, 1)], pan0_sem)
    b = mypan_ref[0]
    for j in range(NB):
        rows = [jnp.sum(vec_ref[k] * b, axis=0, keepdims=True) for k in range(j)]
        rows += [jnp.zeros((1, LANES), F32)] * (NB - j)
        rows.append(jnp.sum(b * b, axis=0, keepdims=True))
        rows.append(jnp.where(col == 0, b[0:1, :], F32(0.0)))
        rows += [jnp.zeros((1, LANES), F32)] * (STATS - NB - 2)
        stat = jnp.concatenate(rows, axis=0)
        stat_ref[j] = stat
        stats_ref[j, pl.ds(col, 1)] = stat[None]
        peers_of_row(
            0,
            lambda to_row, to_col: send(
                stat_ref.at[j], stats_ref.at[j, col], stat_send, stat_sem.at[j],
                to_row, to_col,
            ),
            True,
        )
        matvec(j, b)
        spread(lambda h: part_ref.at[j, h], got_ref.at[j, col], part_send, part_sem.at[j])

        expect(stats_ref.at[j, pl.ds(0, ncol - 1)], stat_sem.at[j])
        stat = stats_ref[j, 0]
        for i in range(1, ncol):
            stat = stat + stats_ref[j, i]
        sums = jnp.sum(stat, axis=1, keepdims=True)
        inner = [sums[k : k + 1, :] for k in range(j)]
        top = stat[NB + 1 : NB + 2, :]
        weight = []
        for m in range(j):
            value = factor[0][m] * inner[0]
            for k in range(1, m + 1):
                value = value + factor[k][m] * inner[k]
            weight.append(value)
        for m in range(j):
            top = top - tops[m] * weight[m]
        above = jnp.where(lane <= j, top, F32(0.0))
        square = sums[NB : NB + 1, :] - jnp.sum(above * above, axis=1, keepdims=True)
        norm = jnp.sqrt(square)
        alpha = top[:, j + 1 : j + 2]
        signed = jnp.where(alpha >= 0, norm, -norm)
        scale = 1.0 / jnp.sqrt(norm * (norm + jnp.abs(alpha)))
        u = b
        for m in range(j):
            u = u - vec_ref[m] * weight[m]
        u = jnp.where(ids > j, u, F32(0.0)) + jnp.where(ids == j + 1, signed, F32(0.0))
        u = u * scale
        vec_ref[j] = u
        publish(vec_ref.at[j], refl_ref, j, v_send, v_sem)
        vtop = jnp.where(lane > j, top, F32(0.0))
        vtop = (vtop + jnp.where(lane == j + 1, signed, F32(0.0))) * scale
        couple = []
        for k in range(j):
            value = inner[k]
            for m in range(j):
                value = value - gram[k][m] * weight[m]
            fix = jnp.where(lane == j + 1, signed, F32(0.0)) - above
            value = value + jnp.sum(tops[k] * fix, axis=1, keepdims=True)
            couple.append(value * scale)
        for k in range(j):
            value = factor[k][k] * couple[k]
            for m in range(k + 1, j):
                value = value + factor[k][m] * couple[m]
            factor[k][j] = -value
            gram[k][j] = couple[k]
            gram[j][k] = couple[k]
        factor[j][j] = jnp.ones((1, 1), F32)
        gram[j][j] = jnp.full((1, 1), 2.0, F32)
        tops.append(vtop)
        hrow = jnp.where(lane == j + 1, -signed, above)
        hess_ref[j, 0, 0:1, :] = jnp.where(row == 0, hrow, F32(0.0))
        if j == 0:
            expect(mypan_ref.at[pl.ds(1, NB)], pan_sem)
        drop = jnp.zeros((tiles, LANES), F32)
        for k in range(j):
            drop = drop + images[k] * weight[k]
        for i in range(j + 1):
            drop = drop + mypan_ref[i] * top[:, i : i + 1]
        drop = drop - mypan_ref[j + 1] * signed
        back = jnp.zeros((tiles, LANES), F32)
        for k in range(j):
            back = back + yvec_ref[k] * couple[k]
        if j + 1 < NB:
            rest = mypan_ref[j + 1]
            for k in range(j):
                rest = rest - yvec_ref[k] * tops[k][:, j + 1 : j + 2]

        expect(got_ref.at[j], part_sem.at[j])
        image = got_ref[j, 0]
        for i in range(1, ncol):
            image = image + got_ref[j, i]
        image = (image - drop) * scale
        images.append(image)
        new_y = image - back
        yvec_ref[j] = new_y
        if j + 1 < NB:
            b = rest - new_y * vtop[:, j + 1 : j + 2]
        publish(yvec_ref.at[j], wy_ref, j, y_send, y_sem)

    at_row = lax.broadcasted_iota(jnp.int32, (NB, NB), 0)
    at_col = lax.broadcasted_iota(jnp.int32, (NB, NB), 1)
    fac = jnp.zeros((NB, NB), F32)
    for k in range(NB):
        for m in range(k, NB):
            here = jnp.logical_and(at_row == k, at_col == m)
            fac = jnp.where(here, jnp.broadcast_to(factor[k][m], (NB, NB)), fac)
    fac_ref[...] = fac

    expect(refl_ref, v_sem)
    expect(wy_ref, y_sem)
    settle(got_ref, part_send, owner == row)
    settle(refl_ref, v_send, home)
    settle(wy_ref, y_send, home)
    expect(stats_ref.at[:, pl.ds(0, ncol - 1)], stat_send)

    @pl.when(col == 0)
    def _():
        settle(got_ref.at[pl.ds(0, 1)], pan0_send, row == 0)
        settle(got_ref, pan_send, row == 0)


def shards(nrow, ncol, matrix):
    rows_local, cols_local = matrix.shape
    tiles = cols_local // LANES
    split = rows_local // cols_local
    blocks = rows_local // BLOCK
    panel = jax.ShapeDtypeStruct((NB, split, tiles, LANES), F32)
    vmem = pl.BlockSpec(memory_space=pltpu.VMEM)
    dma = pltpu.SemaphoreType.DMA
    hess, refl, wy, fac = pl.pallas_call(
        functools.partial(kernel, nrow, ncol),
        out_shape=(panel, panel, panel, jax.ShapeDtypeStruct((NB, NB), F32)),
        in_specs=[pl.BlockSpec(memory_space=pl.ANY)],
        out_specs=(vmem, vmem, vmem, vmem),
        scratch_shapes=[
            pltpu.VMEM((rows_local, cols_local), F32),
            pltpu.VMEM((rows_local, LANES), F32),
            pltpu.VMEM((NB + 1, split, tiles, LANES), F32),
            pltpu.VMEM((NB + 1, tiles, LANES), F32),
            pltpu.VMEM((NB, split, tiles, LANES), F32),
            pltpu.VMEM((NB, ncol, tiles, LANES), F32),
            pltpu.VMEM((NB, STATS, LANES), F32),
            pltpu.VMEM((NB, ncol, STATS, LANES), F32),
            pltpu.VMEM((NB, tiles, LANES), F32),
            pltpu.VMEM((NB, tiles, LANES), F32),
            dma((blocks,)),
            dma(()),
            dma(()),
            dma(()),
            dma(()),
            dma(()),
            dma(()),
            dma((NB,)),
            dma(()),
            dma((NB,)),
            dma(()),
            dma(()),
            dma(()),
            dma(()),
        ],
        compiler_params=pltpu.CompilerParams(
            collective_id=0, has_side_effects=True, vmem_limit_bytes=56 * 2**20
        ),
    )(matrix)

    def lay(x):
        return x.reshape(NB, rows_local).T

    return lay(hess), lay(refl), lay(wy), fac


def solution(mesh):
    nrow, ncol = mesh.shape["row"], mesh.shape["col"]
    return jax.shard_map(
        functools.partial(shards, nrow, ncol),
        mesh=mesh,
        in_specs=(P("row", "col"),),
        out_specs=(P("row", None), P("row", None), P("row", None), P()),
        check_vma=False,
    )
```

```python
import functools

import jax
import jax.numpy as jnp
from jax import lax
from jax.experimental import pallas as pl
from jax.experimental.pallas import tpu as pltpu
from jax.sharding import PartitionSpec as P

NB = 8
LANES = 128
SUB = 8
STATS = 16
BLOCK = 256
F32 = jnp.float32
BF16 = jnp.bfloat16


def kernel(
    nrow, ncol, a_hbm, hess_ref, refl_ref, wy_ref, fac_ref,
    a_ref, first_ref, pan_ref, mypan_ref, part_ref, got_ref, stat_ref, stats_ref,
    vec_ref, yvec_ref,
    load_sem, first_sem, pan0_send, pan0_sem, pan_send, pan_sem, stat_send, stat_sem,
    part_send, part_sem, v_send, v_sem, y_send, y_sem,
):
    rows_local, cols_local = a_hbm.shape
    tiles = cols_local // LANES
    lines = rows_local // LANES
    split = rows_local // cols_local
    row, col = lax.axis_index("row"), lax.axis_index("col")
    blocks = rows_local // BLOCK

    def wrap(value, bound):
        return jnp.where(value >= bound, value - bound, value)

    def peers_of_row(dr, act, skip):
        to_row = wrap(row + dr, nrow)
        for dc in range(1 if skip else 0, ncol):
            act(to_row, wrap(col + dc, ncol))

    def block_load(i):
        span = pl.ds(i * BLOCK, BLOCK)
        return pltpu.make_async_copy(a_hbm.at[span], a_ref.at[span], load_sem.at[i])

    head = pltpu.make_async_copy(a_hbm.at[:, pl.ds(0, LANES)], first_ref, first_sem)

    @pl.when(col == 0)
    def _():
        head.start()

    for i in range(blocks):
        block_load(i).start(priority=1)

    barrier = pltpu.get_barrier_semaphore()

    def greet(to_row, to_col):
        pl.semaphore_signal(
            barrier, inc=1, device_id=(to_row, to_col),
            device_id_type=pl.DeviceIdType.MESH,
        )

    def greet_row(dr, carry):
        peers_of_row(dr, greet, False)
        return carry

    lax.fori_loop(1, nrow, greet_row, 0)
    peers_of_row(0, greet, True)

    def send(src, dst, send_sem, recv_sem, to_row, to_col):
        pltpu.make_async_remote_copy(
            src_ref=src, dst_ref=dst, send_sem=send_sem, recv_sem=recv_sem,
            device_id=(to_row, to_col), device_id_type=pl.DeviceIdType.MESH,
        ).start()

    def place(src, dst, send_sem, recv_sem, to_row, to_col, here):
        @pl.when(here)
        def _():
            pltpu.make_async_copy(src, dst, recv_sem).start()

        @pl.when(jnp.logical_not(here))
        def _():
            send(src, dst, send_sem, recv_sem, to_row, to_col)

    def expect(ref, sem):
        pltpu.make_async_copy(ref, ref, sem).wait()

    def settle(ref, sem, here):
        count = ref.shape[1]

        @pl.when(jnp.logical_not(here))
        def _():
            expect(ref, sem)

        if count > 1:
            @pl.when(here)
            def _():
                expect(ref.at[:, pl.ds(0, count - 1)], sem)

    def spread(piece_of, dst, send_sem, recv_sem):
        for h in range(split):
            to_col = row * split + h
            for dr in range(nrow - 1, 0, -1):
                send(piece_of(h), dst, send_sem, recv_sem, wrap(row + dr, nrow), to_col)
            place(piece_of(h), dst, send_sem, recv_sem, row, to_col, to_col == col)

    @pl.when(col == 0)
    def _():
        head.wait()
        for h in range(split):
            def turn(t, carry):
                at = pl.multiple_of(h * cols_local + t * LANES, LANES)
                block = first_ref[pl.ds(at, LANES), :].T
                for k in range(NB + 1):
                    pan_ref[k, h, pl.ds(t, 1), :] = block[k : k + 1, :]
                return carry

            lax.fori_loop(0, tiles, turn, 0)

    pl.semaphore_wait(barrier, nrow * ncol - 1)

    @pl.when(col == 0)
    def _():
        spread(
            lambda h: pan_ref.at[pl.ds(0, 1), h], mypan_ref.at[pl.ds(0, 1)],
            pan0_send, pan0_sem,
        )
        spread(
            lambda h: pan_ref.at[pl.ds(1, NB), h], mypan_ref.at[pl.ds(1, NB)],
            pan_send, pan_sem,
        )

    ones = jnp.ones((SUB, 2 * LANES), BF16)

    def fold(acc, t, j):
        high = acc.astype(BF16)
        low = (acc - high.astype(F32)).astype(BF16)
        both = jnp.concatenate([high, low], axis=1)
        res = lax.dot_general(
            ones, both, (((1,), (1,)), ((), ())), preferred_element_type=F32
        )
        h = t // tiles
        part_ref[j, h, pl.ds(t - h * tiles, 1), :] = res[0:1, :]

    def matvec(j, vector):
        pieces = [
            jnp.broadcast_to(vector[t : t + 1, :], (SUB, LANES)) for t in range(tiles)
        ]

        def product(t):
            accs = []
            for s in range(LANES // SUB):
                at = pl.ds(pl.multiple_of(t * LANES + s * SUB, SUB), SUB)
                acc = a_ref[at, pl.ds(0, LANES)] * pieces[0]
                for p in range(1, tiles):
                    acc = acc + a_ref[at, pl.ds(p * LANES, LANES)] * pieces[p]
                accs.append(acc)
            return jnp.concatenate(accs, axis=0)

        per = BLOCK // LANES
        if j == 0:
            def loaded(i, carry):
                block_load(i).wait()
                for k in range(per):
                    fold(product(i * per + k), i * per + k, j)
                return carry

            lax.fori_loop(0, blocks, loaded, 0)
        else:
            def step(t, acc):
                fold(acc, t - 1, j)
                return product(t)

            fold(lax.fori_loop(1, lines, step, product(0)), lines - 1, j)

    owner = col // split
    slot = col - owner * split
    home = jnp.logical_and(owner == row, lax.rem(col, nrow) == row)

    def publish(src, ref, j, send_sem, recv_sem):
        for i in range(split):
            to_col = row + nrow * i
            here = jnp.logical_and(owner == row, to_col == col)
            place(src, ref.at[j, slot], send_sem, recv_sem, owner, to_col, here)

    lane = lax.broadcasted_iota(jnp.int32, (1, LANES), 1)
    line_ids = lax.broadcasted_iota(jnp.int32, (tiles, LANES), 0) * LANES
    ids = line_ids + lax.broadcasted_iota(jnp.int32, (tiles, LANES), 1)
    ids = ids + col * cols_local
    hess_ref[...] = jnp.zeros_like(hess_ref)

    factor = [[None] * NB for _ in range(NB)]
    gram = [[None] * NB for _ in range(NB)]
    tops = []
    images = []
    expect(mypan_ref.at[pl.ds(0, 1)], pan0_sem)
    b = mypan_ref[0]
    for j in range(NB):
        rows = [jnp.sum(vec_ref[k] * b, axis=0, keepdims=True) for k in range(j)]
        rows += [jnp.zeros((1, LANES), F32)] * (NB - j)
        rows.append(jnp.sum(b * b, axis=0, keepdims=True))
        rows.append(jnp.where(col == 0, b[0:1, :], F32(0.0)))
        rows += [jnp.zeros((1, LANES), F32)] * (STATS - NB - 2)
        stat = jnp.concatenate(rows, axis=0)
        stat_ref[j] = stat
        stats_ref[j, pl.ds(col, 1)] = stat[None]
        peers_of_row(
            0,
            lambda to_row, to_col: send(
                stat_ref.at[j], stats_ref.at[j, col], stat_send, stat_sem.at[j],
                to_row, to_col,
            ),
            True,
        )
        if j > 0:
            publish(vec_ref.at[j - 1], refl_ref, j - 1, v_send, v_sem)
            publish(yvec_ref.at[j - 1], wy_ref, j - 1, y_send, y_sem)
        matvec(j, b)
        spread(lambda h: part_ref.at[j, h], got_ref.at[j, col], part_send, part_sem.at[j])

        expect(stats_ref.at[j, pl.ds(0, ncol - 1)], stat_sem.at[j])
        stat = stats_ref[j, 0]
        for i in range(1, ncol):
            stat = stat + stats_ref[j, i]
        sums = jnp.sum(stat, axis=1, keepdims=True)
        inner = [sums[k : k + 1, :] for k in range(j)]
        top = stat[NB + 1 : NB + 2, :]
        weight = []
        for m in range(j):
            value = factor[0][m] * inner[0]
            for k in range(1, m + 1):
                value = value + factor[k][m] * inner[k]
            weight.append(value)
        for m in range(j):
            top = top - tops[m] * weight[m]
        above = jnp.where(lane <= j, top, F32(0.0))
        square = sums[NB : NB + 1, :] - jnp.sum(above * above, axis=1, keepdims=True)
        norm = jnp.sqrt(square)
        alpha = top[:, j + 1 : j + 2]
        signed = jnp.where(alpha >= 0, norm, -norm)
        scale = 1.0 / jnp.sqrt(norm * (norm + jnp.abs(alpha)))
        u = b
        for m in range(j):
            u = u - vec_ref[m] * weight[m]
        u = jnp.where(ids > j, u, F32(0.0)) + jnp.where(ids == j + 1, signed, F32(0.0))
        u = u * scale
        vec_ref[j] = u
        vtop = jnp.where(lane > j, top, F32(0.0))
        vtop = (vtop + jnp.where(lane == j + 1, signed, F32(0.0))) * scale
        couple = []
        for k in range(j):
            value = inner[k]
            for m in range(j):
                value = value - gram[k][m] * weight[m]
            fix = jnp.where(lane == j + 1, signed, F32(0.0)) - above
            value = value + jnp.sum(tops[k] * fix, axis=1, keepdims=True)
            couple.append(value * scale)
        for k in range(j):
            value = factor[k][k] * couple[k]
            for m in range(k + 1, j):
                value = value + factor[k][m] * couple[m]
            factor[k][j] = -value
            gram[k][j] = couple[k]
            gram[j][k] = couple[k]
        factor[j][j] = jnp.ones((1, 1), F32)
        gram[j][j] = jnp.full((1, 1), 2.0, F32)
        tops.append(vtop)
        hrow = jnp.where(lane == j + 1, -signed, above)
        hess_ref[j, 0, 0:1, :] = jnp.where(row == 0, hrow, F32(0.0))
        if j == 0:
            expect(mypan_ref.at[pl.ds(1, NB)], pan_sem)
        drop = jnp.zeros((tiles, LANES), F32)
        for k in range(j):
            drop = drop + images[k] * weight[k]
        for i in range(j + 1):
            drop = drop + mypan_ref[i] * top[:, i : i + 1]
        drop = drop - mypan_ref[j + 1] * signed
        back = jnp.zeros((tiles, LANES), F32)
        for k in range(j):
            back = back + yvec_ref[k] * couple[k]
        if j + 1 < NB:
            rest = mypan_ref[j + 1]
            for k in range(j):
                rest = rest - yvec_ref[k] * tops[k][:, j + 1 : j + 2]

        expect(got_ref.at[j], part_sem.at[j])
        image = got_ref[j, 0]
        for i in range(1, ncol):
            image = image + got_ref[j, i]
        image = (image - drop) * scale
        images.append(image)
        if j + 1 == NB:
            publish(vec_ref.at[j], refl_ref, j, v_send, v_sem)
        new_y = image - back
        yvec_ref[j] = new_y
        if j + 1 < NB:
            b = rest - new_y * vtop[:, j + 1 : j + 2]

    publish(yvec_ref.at[NB - 1], wy_ref, NB - 1, y_send, y_sem)
    at_row = lax.broadcasted_iota(jnp.int32, (NB, NB), 0)
    at_col = lax.broadcasted_iota(jnp.int32, (NB, NB), 1)
    fac = jnp.zeros((NB, NB), F32)
    for k in range(NB):
        for m in range(k, NB):
            here = jnp.logical_and(at_row == k, at_col == m)
            fac = jnp.where(here, jnp.broadcast_to(factor[k][m], (NB, NB)), fac)
    fac_ref[...] = fac

    expect(refl_ref, v_sem)
    expect(wy_ref, y_sem)
    settle(got_ref, part_send, owner == row)
    settle(refl_ref, v_send, home)
    settle(wy_ref, y_send, home)
    expect(stats_ref.at[:, pl.ds(0, ncol - 1)], stat_send)

    @pl.when(col == 0)
    def _():
        settle(got_ref.at[pl.ds(0, 1)], pan0_send, row == 0)
        settle(got_ref, pan_send, row == 0)


def finish(hess_in, refl_in, wy_in, fac_in, hess_out, refl_out, wy_out, fac_out):
    split, tiles = hess_in.shape[1:3]
    for src, dst in ((hess_in, hess_out), (refl_in, refl_out), (wy_in, wy_out)):
        for h in range(split):
            for t in range(tiles):
                span = pl.ds((h * tiles + t) * LANES, LANES)
                for k in range(NB):
                    dst[k : k + 1, span] = src[k, h, t : t + 1, :]
    fac_out[...] = fac_in[...]


def shards(nrow, ncol, matrix):
    rows_local, cols_local = matrix.shape
    tiles = cols_local // LANES
    split = rows_local // cols_local
    blocks = rows_local // BLOCK
    panel = jax.ShapeDtypeStruct((NB, split, tiles, LANES), F32)
    vmem = pl.BlockSpec(memory_space=pltpu.VMEM)
    dma = pltpu.SemaphoreType.DMA
    hess, refl, wy, fac = pl.pallas_call(
        functools.partial(kernel, nrow, ncol),
        out_shape=(panel, panel, panel, jax.ShapeDtypeStruct((NB, NB), F32)),
        in_specs=[pl.BlockSpec(memory_space=pl.ANY)],
        out_specs=(vmem, vmem, vmem, vmem),
        scratch_shapes=[
            pltpu.VMEM((rows_local, cols_local), F32),
            pltpu.VMEM((rows_local, LANES), F32),
            pltpu.VMEM((NB + 1, split, tiles, LANES), F32),
            pltpu.VMEM((NB + 1, tiles, LANES), F32),
            pltpu.VMEM((NB, split, tiles, LANES), F32),
            pltpu.VMEM((NB, ncol, tiles, LANES), F32),
            pltpu.VMEM((NB, STATS, LANES), F32),
            pltpu.VMEM((NB, ncol, STATS, LANES), F32),
            pltpu.VMEM((NB, tiles, LANES), F32),
            pltpu.VMEM((NB, tiles, LANES), F32),
            dma((blocks,)),
            dma(()),
            dma(()),
            dma(()),
            dma(()),
            dma(()),
            dma(()),
            dma((NB,)),
            dma(()),
            dma((NB,)),
            dma(()),
            dma(()),
            dma(()),
            dma(()),
        ],
        compiler_params=pltpu.CompilerParams(
            collective_id=0, has_side_effects=True, vmem_limit_bytes=56 * 2**20
        ),
    )(matrix)

    flat = jax.ShapeDtypeStruct((NB, rows_local), F32)
    hess, refl, wy, fac = pl.pallas_call(
        finish,
        out_shape=(flat, flat, flat, jax.ShapeDtypeStruct((NB, NB), F32)),
        in_specs=[vmem] * 4,
        out_specs=(vmem,) * 4,
    )(hess, refl, wy, fac)
    return hess.T, refl.T, wy.T, fac


def solution(mesh):
    nrow, ncol = mesh.shape["row"], mesh.shape["col"]
    return jax.shard_map(
        functools.partial(shards, nrow, ncol),
        mesh=mesh,
        in_specs=(P("row", "col"),),
        out_specs=(P("row", None), P("row", None), P("row", None), P()),
        check_vma=False,
    )
```
